256 devices in a mesh: dp: 128 (over z_hi, x, y, core), query: 2 (over z_lo).
Axes of the slice: x: 4, y: 4, z: 8 (z_hi: 4, z_lo: 2; z = z_hi * 2 + z_lo), core: 2. Of those that a mesh axis runs over, the one named last changes fastest.
Arguments:
- hidden_acts: bfloat16 [16384, 4, 14336], P(('dp', 'query')), may hold values from -5 to 5
- out_grads: bfloat16 [16384, 4, 4096], P(('dp', 'query')), may hold values from -5 to 5
- loss_mask: int32 [16384, 4], P(('dp', 'query')), may hold values from 0 to 1, as said below
- proj_in: bfloat16 [32, 14336], replicated, may hold values from -0.046875 to 0.046875
- proj_out: bfloat16 [32, 4096], replicated, may hold values from -0.09375 to 0.09375
- queries: float32 [256, 1024], P('query'), may hold values from -0.3125 to 0.3125
Outputs:
- scores: float32 [16384, 256], P(('dp', 'query'))
The draws below stay inside these ranges and needn't reach their ends.
Inputs may be any that keep to these rules, and one draw needn't show every extreme that they name: `loss_mask`: the first token of every sequence counts.
All inputs are finite; a program needn't handle non-finite values.
Results may differ from the reference program's by a relative error of at most 0.0007.
Values sent between devices are 32-bit elements; how exact they have to be, the bound alone decides.
No kernel may reach another device: no remote copies, remote signals or barrier semaphores. Data moves between devices by JAX's collectives and lax.ppermute only.
A program may use at most 128 MiB of HBM per device.

```python
import jax
import jax.numpy as jnp
from jax import lax

D = 4096
FF = 14336
P_IN = 32
P_OUT = 32
K = 1024
SEQ_LEN = 4
QUERIES = 256
SEQS = 16384


def draw_loss_mask(key, part):
    position = jnp.arange(SEQS, dtype=jnp.int32)
    live_level = 300 + 600 * position // SEQS
    drawn_ints = jax.random.randint(key, (SEQS, SEQ_LEN), 0, 1000, dtype=jnp.int32)
    is_live = (drawn_ints < live_level[:, None]).astype(jnp.int32)
    leading = (jnp.arange(SEQ_LEN, dtype=jnp.int32) == 0)[None, :]
    return jnp.where(leading, 1, is_live).astype(jnp.int32)


def group_count():
    return max(1, P_IN * P_OUT // 16)


def group_labels(base_key):
    return jax.random.randint(jax.random.fold_in(base_key, 101), (SEQS,), 0, group_count(), dtype=jnp.int32)


def grouped_rows(base_key, row_width, salt_value):
    groups = group_count()
    labels = group_labels(base_key)
    side_key = jax.random.fold_in(base_key, salt_value)
    direction_key, mixing_key, ladder_key, jitter_key = jax.random.split(side_key, 4)
    directions = jax.random.normal(direction_key, (groups, 4, row_width), jnp.float32)
    ladder = jax.random.permutation(ladder_key, groups).astype(jnp.float32) / max(groups - 1, 1)
    scales = 0.45 * jnp.exp(ladder * jnp.log(1.6 / 0.45))
    mixing = 0.5 * jax.random.normal(mixing_key, (SEQS, SEQ_LEN, 4), jnp.float32)
    mixing = mixing * scales[labels][:, None, None]
    blocks = 16 if SEQS % 16 == 0 else 1
    block_rows = SEQS // blocks

    def one_block(inputs):
        mixing_part, label_part, position = inputs
        picked = directions[label_part]
        combined = jnp.einsum('stj,sjw->stw', mixing_part, picked)
        part_key = jax.random.fold_in(jitter_key, position)
        jitter = 0.1 * jax.random.normal(part_key, combined.shape, jnp.float32)
        return jnp.clip(combined + jitter, -5.0, 5.0).astype(jnp.bfloat16)
    stacked = lax.map(one_block, (mixing.reshape(blocks, block_rows, SEQ_LEN, 4), labels.reshape(blocks, block_rows), jnp.arange(blocks, dtype=jnp.int32)))
    return stacked.reshape(SEQS, SEQ_LEN, row_width)


def draw_hidden_acts(key, part):
    return grouped_rows(key, FF, 202)


def draw_out_grads(key, part):
    return grouped_rows(key, D, 303)


def steps_of(stream_key, extent, cuts, smallest, largest):
    level = 1.0
    for axis_at, parts in cuts:
        steps = jax.random.uniform(jax.random.fold_in(jax.random.fold_in(stream_key, 6), axis_at), (parts,), jnp.float32, smallest / len(cuts), largest / len(cuts))
        level = level * jnp.repeat(jnp.exp(steps), extent[axis_at] // parts).reshape((-1,) + (1,) * (len(extent) - 1 - axis_at))
    return level


def normal_values(rng, shape, deviation, bound, shards=(), kind=jnp.bfloat16):
    gain = steps_of(rng, shape, shards, -0.22, 0.18) if shards else 1.0
    array = jax.random.normal(rng, shape, jnp.float32) * deviation * gain
    return jnp.minimum(jnp.maximum(array, -bound), bound).astype(kind)


def setup_inputs(seed: int = 0) -> dict:
    streams_of = jax.random.split(jax.random.key(seed), 7)
    return {
        "hidden_acts": draw_hidden_acts(jax.random.fold_in(streams_of[6], 71), 0),
        "out_grads": draw_out_grads(jax.random.fold_in(streams_of[6], 71), 0),
        "loss_mask": draw_loss_mask(jax.random.fold_in(streams_of[6], 71), 0),
        "proj_in": normal_values(streams_of[3], (P_IN, FF), FF ** -0.5, 0.046875),
        "proj_out": normal_values(streams_of[4], (P_OUT, D), D ** -0.5, 0.09375),
        "queries": normal_values(streams_of[5], (QUERIES, K), (0.7 * K ** -0.5), 0.3125, ((0, 2),), jnp.float32),
    }


def damped_solve(factor, columns):
    halfway = jax.scipy.linalg.solve_triangular(factor, columns, lower=True)
    return jax.scipy.linalg.solve_triangular(factor, halfway, lower=True, trans=1)

def reference(hidden_acts, out_grads, loss_mask, proj_in, proj_out, queries):
    is_live = loss_mask.astype(jnp.float32)
    token_total = jnp.sum(is_live)
    act_proj = lax.dot_general(hidden_acts.reshape(-1, FF).astype(jnp.float32), proj_in.astype(jnp.float32), (((1,), (1,)), ((), ())), preferred_element_type=jnp.float32).reshape(SEQS, SEQ_LEN, P_IN)
    grad_proj = lax.dot_general(out_grads.reshape(-1, D).astype(jnp.float32), proj_out.astype(jnp.float32), (((1,), (1,)), ((), ())), preferred_element_type=jnp.float32).reshape(SEQS, SEQ_LEN, P_OUT)
    weighted = grad_proj * is_live[:, :, None]
    outer = jnp.einsum('stg,stx->sgx', weighted, act_proj, precision=lax.Precision.HIGHEST).reshape(SEQS, K)
    sketch = outer / token_total
    fisher = lax.dot_general(sketch, sketch, (((0,), (0,)), ((), ())), precision=lax.Precision.HIGHEST)
    damping = 0.1 * jnp.trace(fisher) / K
    system = fisher + damping * jnp.eye(K, dtype=jnp.float32)
    factor = jnp.linalg.cholesky(system)
    solved = damped_solve(factor, queries.T)
    return jnp.dot(sketch, solved, precision=lax.Precision.HIGHEST)
```

```python
import functools

import jax
import jax.numpy as jnp
from jax import lax
from jax.experimental import pallas as pl
from jax.experimental.pallas import tpu as pltpu
from jax.sharding import Mesh
from jax.sharding import PartitionSpec as P

K = 1024
TILE = 128
SIDE = K // TILE
PACKED = SIDE * (SIDE + 1) // 2
AXES = ("z_hi", "x", "y", "core", "z_lo")
SIZES = {"z_hi": 4, "x": 4, "y": 4, "core": 2, "z_lo": 2}
STAGES = (("core",), ("x", "y"), ("z_hi", "z_lo"))
HI = lax.Precision.HIGHEST


def tile_index(i, j):
    return i * SIDE - i * (i - 1) // 2 + (j - i)


def dot_f32(a, b, dims):
    return lax.dot_general(a, b, (dims, ((), ())), precision=HI, preferred_element_type=jnp.float32)


def gram_body(act_ref, grad_ref, mask_ref, outer_ref, tiles_ref):
    live = mask_ref[...].astype(jnp.float32)
    tokens, width, seqs = act_ref.shape
    weighted = [grad_ref[t] * live[t : t + 1, :] for t in range(tokens)]
    acts = [act_ref[t] for t in range(tokens)]
    for g in range(K // width):
        total = weighted[0][g : g + 1, :] * acts[0]
        for t in range(1, tokens):
            total = total + weighted[t][g : g + 1, :] * acts[t]
        outer_ref[g * width : (g + 1) * width, :] = total
    for i in range(SIDE):
        rows = outer_ref[i * TILE : (i + 1) * TILE, :]
        strip = dot_f32(rows, outer_ref[i * TILE :, :], ((1,), (1,)))
        for j in range(i, SIDE):
            tiles_ref[tile_index(i, j)] = strip[:, (j - i) * TILE : (j - i + 1) * TILE]
    row = lax.broadcasted_iota(jnp.int32, (8, TILE), 0)
    lane = lax.broadcasted_iota(jnp.int32, (8, TILE), 1)
    count = jnp.sum(live)
    tiles_ref[0, 0:8, :] = jnp.where((row == 1) & (lane == 0), count, tiles_ref[0, 0:8, :])


def local_gram(act, grad, mask):
    seqs = act.shape[2]
    return pl.pallas_call(
        gram_body,
        out_shape=(
            jax.ShapeDtypeStruct((K, seqs), jnp.float32),
            jax.ShapeDtypeStruct((PACKED, TILE, TILE), jnp.float32),
        ),
        name="local_gram",
    )(act, grad, mask)


def invert_factor(src, dst):
    lane = lax.broadcasted_iota(jnp.int32, (8, TILE), 1)
    sub = lax.broadcasted_iota(jnp.int32, (8, TILE), 0)
    groups = TILE // 8
    for g in range(groups):
        tiles = [src[8 * q : 8 * q + 8, :] for q in range(g, groups)]
        cols = [
            [jnp.broadcast_to(t[:, 8 * g + j : 8 * g + j + 1], (8, TILE)) for t in tiles]
            for j in range(8)
        ]
        inside = (lane >= 8 * g) & (lane < 8 * g + 8)
        tiles = [jnp.where(inside, 0.0, t) for t in tiles]
        tiles[0] = jnp.where(lane == sub + 8 * g, 1.0, tiles[0])
        scale = jnp.zeros((8, TILE), jnp.float32)
        for j in range(8):
            pivot = jnp.broadcast_to(cols[j][0][j : j + 1, :], (8, TILE))
            inverse = 1.0 / pivot
            row = jnp.broadcast_to(tiles[0][j : j + 1, :], (8, TILE))
            root = lax.rsqrt(pivot)
            root = root * (1.5 - 0.5 * (pivot * root) * root)
            scale = jnp.where(sub == j, root, scale)
            factors = [c * inverse for c in cols[j]]
            factors[0] = jnp.where(sub > j, factors[0], 0.0)
            for l in range(j + 1, 8):
                top = jnp.broadcast_to(cols[l][0][j : j + 1, :], (8, TILE))
                cols[l] = [c - m * top for c, m in zip(cols[l], factors)]
            tiles = [t - m * row for t, m in zip(tiles, factors)]
        dst[8 * g : 8 * g + 8, :] = jnp.where(lane <= sub + 8 * g, tiles[0] * scale, 0.0)
        for q in range(1, len(tiles)):
            src[8 * (g + q) : 8 * (g + q) + 8, :] = tiles[q]


def solve_body(tiles_ref, query_ref, outer_ref, out_ref, a_ref, t_ref, l_ref, b_ref):
    queries = query_ref.shape[1]
    a_ref[...] = tiles_ref[...]
    b_ref[:, :queries] = query_ref[...]
    b_ref[:, queries:] = outer_ref[...]
    row = lax.broadcasted_iota(jnp.int32, (TILE, TILE), 0)
    lane = lax.broadcasted_iota(jnp.int32, (TILE, TILE), 1)
    eye = row == lane
    first = a_ref[0]
    holds_count = (row == 1) & (lane == 0)
    token_total = jnp.sum(jnp.where(holds_count, first, 0.0))
    twin = jnp.sum(jnp.where((row == 0) & (lane == 1), first, 0.0))
    a_ref[0] = jnp.where(holds_count, twin, first)
    trace = jnp.zeros((8, TILE), jnp.float32)
    for i in range(SIDE):
        diagonal = jnp.where(eye, a_ref[tile_index(i, i)], 0.0)
        trace = trace + jnp.sum(diagonal.reshape(TILE // 8, 8, TILE), axis=0)
    damping = 0.1 * jnp.sum(trace) / K
    for i in range(SIDE):
        a_ref[tile_index(i, i)] = a_ref[tile_index(i, i)] + jnp.where(eye, damping, 0.0)
    out_ref[...] = jnp.zeros_like(out_ref)

    def eliminate(k):
        inv = l_ref[...]
        rows = {j: dot_f32(inv, a_ref[tile_index(k, j)], ((1,), (0,))) for j in range(k + 1, SIDE)}
        right = dot_f32(inv, b_ref[TILE * k : TILE * (k + 1), :], ((1,), (0,)))
        for j in range(k + 1, SIDE):
            for c in range(j, SIDE):
                a_ref[tile_index(j, c)] -= dot_f32(rows[j], rows[c], ((0,), (0,)))
            b_ref[TILE * j : TILE * (j + 1), :] -= dot_f32(rows[j], right, ((0,), (0,)))
        out_ref[...] += dot_f32(right[:, queries:], right[:, :queries], ((0,), (0,)))

    def step(k, carry):
        t_ref[...] = a_ref[k * SIDE - (k * (k - 1)) // 2]
        invert_factor(t_ref, l_ref)
        for each in range(SIDE):
            pl.when(k == each)(functools.partial(eliminate, each))
        return carry

    lax.fori_loop(0, SIDE, step, 0)
    out_ref[...] = out_ref[...] * token_total


def damped_scores(tiles, queries_t, outer_t):
    queries, seqs = queries_t.shape[1], outer_t.shape[1]
    return pl.pallas_call(
        solve_body,
        out_shape=jax.ShapeDtypeStruct((seqs, queries), jnp.float32),
        scratch_shapes=[
            pltpu.VMEM((PACKED, TILE, TILE), jnp.float32),
            pltpu.VMEM((TILE, TILE), jnp.float32),
            pltpu.VMEM((TILE, TILE), jnp.float32),
            pltpu.VMEM((K, queries + seqs), jnp.float32),
        ],
        name="damped_scores",
    )(tiles, queries_t, outer_t)


def members(axes):
    count = 1
    for axis in axes:
        count *= SIZES[axis]
    return count


def scatter_sum(rows, axes):
    peers = members(axes)
    pieces = rows.reshape(peers, -1, TILE)
    return jnp.sum(lax.all_to_all(pieces, axes, 0, 0, tiled=True), axis=0)


def gather_rows(rows, axes):
    peers = members(axes)
    copies = jnp.broadcast_to(rows[None], (peers, *rows.shape))
    return lax.all_to_all(copies, axes, 0, 0, tiled=True).reshape(-1, TILE)


def summed(tiles):
    rows = tiles.reshape(-1, TILE)
    for axes in STAGES:
        rows = scatter_sum(rows, axes)
    for axes in reversed(STAGES):
        rows = gather_rows(rows, axes)
    return rows.reshape(tiles.shape)


def swap_queries(queries):
    other = lax.ppermute(queries, "z_lo", [(0, 1), (1, 0)])
    return jnp.concatenate([queries, other], axis=0).T


def on_device(hidden_acts, out_grads, loss_mask, proj_in, proj_out, queries):
    queries_t = swap_queries(queries)
    act = lax.dot_general(
        hidden_acts, proj_in, (((2,), (1,)), ((), ())), preferred_element_type=jnp.float32
    )
    grad = lax.dot_general(
        out_grads, proj_out, (((2,), (1,)), ((), ())), preferred_element_type=jnp.float32
    )
    outer_t, tiles = local_gram(act.transpose(1, 2, 0), grad.transpose(1, 2, 0), loss_mask.T)
    tiles = summed(tiles)
    scores = damped_scores(tiles, queries_t, outer_t)
    half = queries.shape[0]
    mine, other = scores[:, :half], scores[:, half:]
    is_first = lax.axis_index("z_lo") == 0
    return jnp.concatenate(
        [jnp.where(is_first, mine, other), jnp.where(is_first, other, mine)], axis=1
    )


def solution(mesh):
    finer = Mesh(mesh.devices.reshape(4, 4, 4, 2, mesh.shape["query"]), AXES)
    in_specs = (
        P(AXES, None, None),
        P(AXES, None, None),
        P(AXES, None),
        P(),
        P(),
        P("z_lo", None),
    )
    return jax.shard_map(
        on_device, mesh=finer, in_specs=in_specs, out_specs=P(AXES, None), check_vma=False
    )
```

```python
import functools

import jax
import jax.numpy as jnp
from jax import lax
from jax.experimental import pallas as pl
from jax.experimental.pallas import tpu as pltpu
from jax.sharding import Mesh
from jax.sharding import PartitionSpec as P

K = 1024
TILE = 128
SIDE = K // TILE
PACKED = SIDE * (SIDE + 1) // 2
HALF = PACKED // 2
STEPS = 4
AXES = ("z_hi", "x", "y", "core", "z_lo")
SIZES = {"z_hi": 4, "x": 4, "y": 4, "core": 2, "z_lo": 2}
STAGES = (("x", "y"), ("z_hi", "z_lo"))
SWAP = [(0, 1), (1, 0)]


def tile_index(i, j):
    return i * SIDE - i * (i - 1) // 2 + (j - i)


def thirds(x):
    hi = x.astype(jnp.bfloat16)
    rest = x - hi.astype(jnp.float32)
    mid = rest.astype(jnp.bfloat16)
    low = (rest - mid.astype(jnp.float32)).astype(jnp.bfloat16)
    return hi, mid, low


def left_parts(parts, axis):
    hi, mid, low = parts
    return jnp.concatenate([low, mid, hi, mid, hi, hi], axis=axis)


def right_parts(parts, axis):
    hi, mid, low = parts
    return jnp.concatenate([hi, mid, low, hi, mid, hi], axis=axis)


def multiply(a, b):
    return jnp.dot(a, b, preferred_element_type=jnp.float32)


def multiply_rows(a, b):
    return lax.dot_general(a, b, (((1,), (1,)), ((), ())), preferred_element_type=jnp.float32)


def project(x_ref, w_ref, seqs, tokens):
    width = w_ref.shape[0]
    fold = TILE * 2 // width
    blocks = w_ref.shape[1] // TILE
    rows = fold * tokens
    per_seq = blocks * tokens
    left = [
        jnp.concatenate([x_ref[per_seq * s + rows * h : per_seq * s + rows * (h + 1), :] for s in range(seqs)], axis=0)
        for h in range(blocks // fold)
    ]
    right = [
        jnp.concatenate([w_ref[:, TILE * (fold * h + c) : TILE * (fold * h + c + 1)] for c in range(fold)], axis=0)
        for h in range(blocks // fold)
    ]
    all_pairs = multiply_rows(jnp.concatenate(left, axis=1), jnp.concatenate(right, axis=1))
    row = lax.broadcasted_iota(jnp.int32, all_pairs.shape, 0)
    lane = lax.broadcasted_iota(jnp.int32, all_pairs.shape, 1)
    matched = jnp.where((row // tokens) % fold == lane // width, all_pairs, 0.0)
    return jnp.sum(matched.reshape(seqs, rows // 8, 8, fold * width), axis=1).reshape(seqs * 8, fold * width)


def by_token(partial, width, tokens):
    fold_lane = lax.broadcasted_iota(jnp.int32, (width, partial.shape[1]), 1)
    fold_row = lax.broadcasted_iota(jnp.int32, (width, partial.shape[1]), 0)
    fold = jnp.where(fold_lane % width == fold_row, 1.0, 0.0).astype(jnp.bfloat16)
    hi, mid, low = thirds(partial)
    folded = multiply_rows(
        jnp.concatenate([fold] * 3, axis=1), jnp.concatenate([low, mid, hi], axis=1)
    )
    row = lax.broadcasted_iota(jnp.int32, (partial.shape[0], tokens * TILE), 0)
    lane = lax.broadcasted_iota(jnp.int32, (partial.shape[0], tokens * TILE), 1)
    pick = (row % tokens == lane // TILE) & (row // 8 == lane % TILE)
    pick = jnp.where(pick, 1.0, 0.0).astype(jnp.bfloat16)
    hi, mid, low = thirds(folded)
    return multiply(jnp.concatenate([low, mid, hi], axis=1), jnp.concatenate([pick] * 3, axis=0))


def gram_body(
    where_ref, act_ref, grad_ref, mask_ref, in_ref, out_ref, outer_ref, kept_ref, sent_ref, a_part, g_part, tiles
):
    tokens = mask_ref.shape[0]
    seqs = outer_ref.shape[1]
    some = seqs // STEPS
    step = pl.program_id(0)
    start = pl.multiple_of(step * some * 8, some * 8)
    a_part[pl.ds(start, some * 8), :] = project(act_ref, in_ref, some, tokens)
    g_part[pl.ds(start, some * 8), :] = project(grad_ref, out_ref, some, tokens)

    @pl.when(step == STEPS - 1)
    def _():
        live = mask_ref[...].astype(jnp.float32)
        width = in_ref.shape[0]
        acts = by_token(a_part[...], width, tokens)
        grads = by_token(g_part[...], out_ref.shape[0], tokens)
        acts = [acts[:, TILE * t : TILE * t + seqs] for t in range(tokens)]
        grads = [grads[:, TILE * t : TILE * t + seqs] * live[t : t + 1, :] for t in range(tokens)]
        for g in range(K // width):
            total = grads[0][g : g + 1, :] * acts[0]
            for t in range(1, tokens):
                total = total + grads[t][g : g + 1, :] * acts[t]
            outer_ref[g * width : (g + 1) * width, :] = total
        parts = thirds(outer_ref[...])
        left, right = left_parts(parts, 1), right_parts(parts, 1)
        for i in range(SIDE):
            strip = multiply_rows(left[TILE * i : TILE * (i + 1), :], right[TILE * i :, :])
            for j in range(i, SIDE):
                tiles[tile_index(i, j)] = strip[:, (j - i) * TILE : (j - i + 1) * TILE]
        row = lax.broadcasted_iota(jnp.int32, (8, TILE), 0)
        lane = lax.broadcasted_iota(jnp.int32, (8, TILE), 1)
        count = jnp.sum(live)
        tiles[0, 0:8, :] = jnp.where((row == 1) & (lane == 0), count, tiles[0, 0:8, :])
        core = where_ref[0]
        kept_ref[...] = tiles[pl.ds(core * HALF, HALF)]
        sent_ref[...] = tiles[pl.ds((1 - core) * HALF, HALF)]


def as_blocks(x):
    seqs, tokens, width = x.shape
    blocks = width // TILE
    return x.reshape(seqs, tokens, blocks, TILE).transpose(0, 2, 1, 3).reshape(seqs * blocks * tokens, TILE)


def local_gram(where, hidden_acts, out_grads, mask_t, proj_in, proj_out):
    seqs = hidden_acts.shape[0]
    acts, grads = as_blocks(hidden_acts), as_blocks(out_grads)

    def whole(shape):
        return pl.BlockSpec(shape, lambda i: (0,) * len(shape))

    half = (HALF, TILE, TILE)
    return pl.pallas_call(
        gram_body,
        grid=(STEPS,),
        in_specs=[
            pl.BlockSpec(memory_space=pltpu.SMEM),
            pl.BlockSpec((acts.shape[0] // STEPS, TILE), lambda i: (i, 0)),
            pl.BlockSpec((grads.shape[0] // STEPS, TILE), lambda i: (i, 0)),
            whole(mask_t.shape),
            whole(proj_in.shape),
            whole(proj_out.shape),
        ],
        out_specs=(whole((K, seqs)), whole(half), whole(half)),
        out_shape=(
            jax.ShapeDtypeStruct((K, seqs), jnp.float32),
            jax.ShapeDtypeStruct(half, jnp.float32),
            jax.ShapeDtypeStruct(half, jnp.float32),
        ),
        scratch_shapes=[
            pltpu.VMEM((seqs * 8, 2 * TILE), jnp.float32),
            pltpu.VMEM((seqs * 8, 2 * TILE), jnp.float32),
            pltpu.VMEM((PACKED, TILE, TILE), jnp.float32),
        ],
        name="local_gram",
    )(where, acts, grads, mask_t, proj_in, proj_out)


def invert_factor(src, dst):
    lane = lax.broadcasted_iota(jnp.int32, (8, TILE), 1)
    sub = lax.broadcasted_iota(jnp.int32, (8, TILE), 0)
    groups = TILE // 8
    for g in range(groups):
        tiles = [src[8 * q : 8 * q + 8, :] for q in range(g, groups)]
        cols = [
            [jnp.broadcast_to(t[:, 8 * g + j : 8 * g + j + 1], (8, TILE)) for t in tiles]
            for j in range(8)
        ]
        inside = (lane >= 8 * g) & (lane < 8 * g + 8)
        tiles = [jnp.where(inside, 0.0, t) for t in tiles]
        tiles[0] = jnp.where(lane == sub + 8 * g, 1.0, tiles[0])
        scale = jnp.zeros((8, TILE), jnp.float32)
        for j in range(8):
            pivot = jnp.broadcast_to(cols[j][0][j : j + 1, :], (8, TILE))
            guess = pl.reciprocal(pivot, approx=True)
            fix = 2.0 - pivot * guess
            inverse = guess * fix
            row = jnp.broadcast_to(tiles[0][j : j + 1, :], (8, TILE))
            root = lax.rsqrt(pivot)
            root = root * (1.5 - 0.5 * (pivot * root) * root)
            scale = jnp.where(sub == j, root, scale)
            lead = jnp.where(sub > j, cols[j][0] * guess, 0.0) * fix
            factors = [lead] + [c * inverse for c in cols[j][1:]]
            for l in range(j + 1, 8):
                top = jnp.broadcast_to(cols[l][0][j : j + 1, :], (8, TILE))
                cols[l] = [c - m * top for c, m in zip(cols[l], factors)]
            tiles = [t - m * row for t, m in zip(tiles, factors)]
        dst[8 * g : 8 * g + 8, :] = jnp.where(lane <= sub + 8 * g, tiles[0] * scale, 0.0)
        for q in range(1, len(tiles)):
            src[8 * (g + q) : 8 * (g + q) + 8, :] = tiles[q]


def solve_body(
    where_ref, mine_ref, other_ref, query_ref, query2_ref, outer_ref, out_ref, a_ref, t_ref, l_ref, b_ref
):
    half = query_ref.shape[0]
    queries = 2 * half
    core = where_ref[0]
    a_ref[pl.ds(core * HALF, HALF)] = mine_ref[...]
    a_ref[pl.ds((1 - core) * HALF, HALF)] = other_ref[...]
    b_ref[:, :half] = query_ref[...].T
    b_ref[:, half:queries] = query2_ref[...].T
    b_ref[:, queries:] = outer_ref[...]
    row = lax.broadcasted_iota(jnp.int32, (TILE, TILE), 0)
    lane = lax.broadcasted_iota(jnp.int32, (TILE, TILE), 1)
    eye = row == lane
    first = a_ref[0]
    holds_count = (row == 1) & (lane == 0)
    token_total = jnp.sum(jnp.where(holds_count, first, 0.0))
    twin = jnp.sum(jnp.where((row == 0) & (lane == 1), first, 0.0))
    a_ref[0] = jnp.where(holds_count, twin, first)
    trace = jnp.zeros((8, TILE), jnp.float32)
    for i in range(SIDE):
        diagonal = jnp.where(eye, a_ref[tile_index(i, i)], 0.0)
        trace = trace + jnp.sum(diagonal.reshape(TILE // 8, 8, TILE), axis=0)
    damping = 0.1 * jnp.sum(trace) / K
    for i in range(SIDE):
        a_ref[tile_index(i, i)] = a_ref[tile_index(i, i)] + jnp.where(eye, damping, 0.0)
    out_ref[...] = jnp.zeros_like(out_ref)

    def eliminate(k):
        right_of = [a_ref[tile_index(k, j)] for j in range(k + 1, SIDE)]
        strip = jnp.concatenate(right_of + [b_ref[TILE * k : TILE * (k + 1), :]], axis=1)
        strip = multiply(left_parts(thirds(l_ref[...]), 1), right_parts(thirds(strip), 0))
        wide = right_parts(thirds(strip), 0)
        width = TILE * (SIDE - 1 - k)

        def flipped(start, stop):
            return left_parts(thirds(strip[:, start:stop].T), 1)

        for j in range(k + 1, SIDE):
            start = TILE * (j - k - 1)
            delta = multiply(flipped(start, start + TILE), wide[:, start:])
            for c in range(j, SIDE):
                a_ref[tile_index(j, c)] -= delta[:, TILE * (c - j) : TILE * (c - j + 1)]
            b_ref[TILE * j : TILE * (j + 1), :] -= delta[:, TILE * (SIDE - j) :]
        out_ref[...] += multiply(flipped(width + queries, strip.shape[1]), wide[:, width : width + queries])

    def step(k, carry):
        t_ref[...] = a_ref[k * SIDE - (k * (k - 1)) // 2]
        invert_factor(t_ref, l_ref)
        for each in range(SIDE):
            pl.when(k == each)(functools.partial(eliminate, each))
        return carry

    lax.fori_loop(0, SIDE, step, 0)
    scores = out_ref[...] * token_total
    is_first = where_ref[1] == 0
    out_ref[:, :half] = jnp.where(is_first, scores[:, :half], scores[:, half:])
    out_ref[:, half:] = jnp.where(is_first, scores[:, half:], scores[:, :half])


def damped_scores(where, mine, other, my_queries, other_queries, outer_t):
    queries, seqs = 2 * my_queries.shape[0], outer_t.shape[1]
    vmem = pl.BlockSpec(memory_space=pltpu.VMEM)
    return pl.pallas_call(
        solve_body,
        in_specs=[pl.BlockSpec(memory_space=pltpu.SMEM), vmem, vmem, vmem, vmem, vmem],
        out_shape=jax.ShapeDtypeStruct((seqs, queries), jnp.float32),
        scratch_shapes=[
            pltpu.VMEM((PACKED, TILE, TILE), jnp.float32),
            pltpu.VMEM((TILE, TILE), jnp.float32),
            pltpu.VMEM((TILE, TILE), jnp.float32),
            pltpu.VMEM((K, queries + seqs), jnp.float32),
        ],
        name="damped_scores",
    )(where, mine, other, my_queries, other_queries, outer_t)


def members(axes):
    count = 1
    for axis in axes:
        count *= SIZES[axis]
    return count


def scatter_sum(rows, axes):
    peers = members(axes)
    pieces = rows.reshape(peers, -1, TILE)
    return jnp.sum(lax.all_to_all(pieces, axes, 0, 0, tiled=True), axis=0)


def gather_rows(rows, axes):
    peers = members(axes)
    copies = jnp.broadcast_to(rows[None], (peers, *rows.shape))
    return lax.all_to_all(copies, axes, 0, 0, tiled=True).reshape(-1, TILE)


def summed(kept, sent):
    rows = (kept + lax.ppermute(sent, "core", SWAP)).reshape(-1, TILE)
    for axes in STAGES:
        rows = scatter_sum(rows, axes)
    for axes in reversed(STAGES):
        rows = gather_rows(rows, axes)
    mine = rows.reshape(kept.shape)
    return mine, lax.ppermute(mine, "core", SWAP)


def on_device(hidden_acts, out_grads, loss_mask, proj_in, proj_out, queries):
    where = jnp.stack([lax.axis_index("core"), lax.axis_index("z_lo")]).astype(jnp.int32)
    other_queries = lax.ppermute(queries, "z_lo", SWAP)
    outer_t, kept, sent = local_gram(where, hidden_acts, out_grads, loss_mask.T, proj_in, proj_out)
    other_queries, kept, sent = lax.optimization_barrier((other_queries, kept, sent))
    mine, other = summed(kept, sent)
    return damped_scores(where, mine, other, queries, other_queries, outer_t)


def solution(mesh):
    finer = Mesh(mesh.devices.reshape(4, 4, 4, 2, mesh.shape["query"]), AXES)
    in_specs = (
        P(AXES, None, None),
        P(AXES, None, None),
        P(AXES, None),
        P(),
        P(),
        P("z_lo", None),
    )
    return jax.shard_map(
        on_device, mesh=finer, in_specs=in_specs, out_specs=P(AXES, None), check_vma=False
    )
```

```python
import functools

import jax
import jax.numpy as jnp
from jax import lax
from jax.experimental import pallas as pl
from jax.experimental.pallas import tpu as pltpu
from jax.sharding import Mesh
from jax.sharding import PartitionSpec as P

K = 1024
TILE = 128
SIDE = K // TILE
PACKED = SIDE * (SIDE + 1) // 2
HALF = PACKED // 2
STEPS = 4
AXES = ("z_hi", "x", "y", "core", "z_lo")
SIZES = {"z_hi": 4, "x": 4, "y": 4, "core": 2, "z_lo": 2}
NEAR = ("x", "y", "z_lo")
SWAP = [(0, 1), (1, 0)]


def tile_index(i, j):
    return i * SIDE - i * (i - 1) // 2 + (j - i)


def thirds(x):
    hi = x.astype(jnp.bfloat16)
    rest = x - hi.astype(jnp.float32)
    mid = rest.astype(jnp.bfloat16)
    low = (rest - mid.astype(jnp.float32)).astype(jnp.bfloat16)
    return hi, mid, low


def left_parts(parts, axis):
    hi, mid, low = parts
    return jnp.concatenate([low, mid, hi, mid, hi, hi], axis=axis)


def right_parts(parts, axis):
    hi, mid, low = parts
    return jnp.concatenate([hi, mid, low, hi, mid, hi], axis=axis)


def multiply(a, b):
    return jnp.dot(a, b, preferred_element_type=jnp.float32)


def multiply_rows(a, b):
    return lax.dot_general(a, b, (((1,), (1,)), ((), ())), preferred_element_type=jnp.float32)


def project(x_ref, w_ref, seqs, tokens):
    width = w_ref.shape[0]
    fold = TILE * 2 // width
    blocks = w_ref.shape[1] // TILE
    rows = fold * tokens
    per_seq = blocks * tokens
    left = [
        jnp.concatenate([x_ref[per_seq * s + rows * h : per_seq * s + rows * (h + 1), :] for s in range(seqs)], axis=0)
        for h in range(blocks // fold)
    ]
    right = [
        jnp.concatenate([w_ref[:, TILE * (fold * h + c) : TILE * (fold * h + c + 1)] for c in range(fold)], axis=0)
        for h in range(blocks // fold)
    ]
    all_pairs = multiply_rows(jnp.concatenate(left, axis=1), jnp.concatenate(right, axis=1))
    row = lax.broadcasted_iota(jnp.int32, all_pairs.shape, 0)
    lane = lax.broadcasted_iota(jnp.int32, all_pairs.shape, 1)
    matched = jnp.where((row // tokens) % fold == lane // width, all_pairs, 0.0)
    return jnp.sum(matched.reshape(seqs, rows // 8, 8, fold * width), axis=1).reshape(seqs * 8, fold * width)


def by_token(partial, width, tokens):
    fold_lane = lax.broadcasted_iota(jnp.int32, (width, partial.shape[1]), 1)
    fold_row = lax.broadcasted_iota(jnp.int32, (width, partial.shape[1]), 0)
    fold = jnp.where(fold_lane % width == fold_row, 1.0, 0.0).astype(jnp.bfloat16)
    hi, mid, low = thirds(partial)
    folded = multiply_rows(
        jnp.concatenate([fold] * 3, axis=1), jnp.concatenate([low, mid, hi], axis=1)
    )
    row = lax.broadcasted_iota(jnp.int32, (partial.shape[0], tokens * TILE), 0)
    lane = lax.broadcasted_iota(jnp.int32, (partial.shape[0], tokens * TILE), 1)
    pick = (row % tokens == lane // TILE) & (row // 8 == lane % TILE)
    pick = jnp.where(pick, 1.0, 0.0).astype(jnp.bfloat16)
    hi, mid, low = thirds(folded)
    return multiply(jnp.concatenate([low, mid, hi], axis=1), jnp.concatenate([pick] * 3, axis=0))


def gram_body(
    act_ref, grad_ref, mask_ref, in_ref, out_ref, outer_ref, kept_ref, sent_ref, a_part, g_part, tiles
):
    tokens = mask_ref.shape[0]
    seqs = outer_ref.shape[1]
    some = seqs // STEPS
    step = pl.program_id(0)
    start = pl.multiple_of(step * some * 8, some * 8)
    a_part[pl.ds(start, some * 8), :] = project(act_ref, in_ref, some, tokens)
    g_part[pl.ds(start, some * 8), :] = project(grad_ref, out_ref, some, tokens)

    @pl.when(step == STEPS - 1)
    def _():
        live = mask_ref[...].astype(jnp.float32)
        width = in_ref.shape[0]
        acts = by_token(a_part[...], width, tokens)
        grads = by_token(g_part[...], out_ref.shape[0], tokens)
        acts = [acts[:, TILE * t : TILE * t + seqs] for t in range(tokens)]
        grads = [grads[:, TILE * t : TILE * t + seqs] * live[t : t + 1, :] for t in range(tokens)]
        for g in range(K // width):
            total = grads[0][g : g + 1, :] * acts[0]
            for t in range(1, tokens):
                total = total + grads[t][g : g + 1, :] * acts[t]
            outer_ref[g * width : (g + 1) * width, :] = total
        parts = thirds(outer_ref[...])
        left, right = left_parts(parts, 1), right_parts(parts, 1)
        for i in range(SIDE):
            strip = multiply_rows(left[TILE * i : TILE * (i + 1), :], right[TILE * i :, :])
            for j in range(i, SIDE):
                tiles[tile_index(i, j)] = strip[:, (j - i) * TILE : (j - i + 1) * TILE]
        row = lax.broadcasted_iota(jnp.int32, (8, TILE), 0)
        lane = lax.broadcasted_iota(jnp.int32, (8, TILE), 1)
        count = jnp.sum(live)
        tiles[0, 0:8, :] = jnp.where((row == 1) & (lane == 0), count, tiles[0, 0:8, :])
        core = lax.axis_index("core")
        kept_ref[...] = tiles[pl.ds(core * HALF, HALF)]
        sent_ref[...] = tiles[pl.ds((1 - core) * HALF, HALF)]


def as_blocks(x):
    seqs, tokens, width = x.shape
    blocks = width // TILE
    return x.reshape(seqs, tokens, blocks, TILE).transpose(0, 2, 1, 3).reshape(seqs * blocks * tokens, TILE)


def local_gram(hidden_acts, out_grads, mask_t, proj_in, proj_out):
    seqs = hidden_acts.shape[0]
    acts, grads = as_blocks(hidden_acts), as_blocks(out_grads)

    def whole(shape):
        return pl.BlockSpec(shape, lambda i: (0,) * len(shape))

    half = (HALF, TILE, TILE)
    return pl.pallas_call(
        gram_body,
        grid=(STEPS,),
        in_specs=[
            pl.BlockSpec((acts.shape[0] // STEPS, TILE), lambda i: (i, 0)),
            pl.BlockSpec((grads.shape[0] // STEPS, TILE), lambda i: (i, 0)),
            whole(mask_t.shape),
            whole(proj_in.shape),
            whole(proj_out.shape),
        ],
        out_specs=(whole((K, seqs)), whole(half), whole(half)),
        out_shape=(
            jax.ShapeDtypeStruct((K, seqs), jnp.float32),
            jax.ShapeDtypeStruct(half, jnp.float32),
            jax.ShapeDtypeStruct(half, jnp.float32),
        ),
        scratch_shapes=[
            pltpu.VMEM((seqs * 8, 2 * TILE), jnp.float32),
            pltpu.VMEM((seqs * 8, 2 * TILE), jnp.float32),
            pltpu.VMEM((PACKED, TILE, TILE), jnp.float32),
        ],
        name="local_gram",
    )(acts, grads, mask_t, proj_in, proj_out)


def invert_factor(src, dst):
    lane = lax.broadcasted_iota(jnp.int32, (8, TILE), 1)
    sub = lax.broadcasted_iota(jnp.int32, (8, TILE), 0)
    groups = TILE // 8
    for g in range(groups):
        tiles = [src[8 * q : 8 * q + 8, :] for q in range(g, groups)]
        cols = [
            [jnp.broadcast_to(t[:, 8 * g + j : 8 * g + j + 1], (8, TILE)) for t in tiles]
            for j in range(8)
        ]
        inside = (lane >= 8 * g) & (lane < 8 * g + 8)
        tiles = [jnp.where(inside, 0.0, t) for t in tiles]
        tiles[0] = jnp.where(lane == sub + 8 * g, 1.0, tiles[0])
        scale = jnp.zeros((8, TILE), jnp.float32)
        for j in range(8):
            pivot = jnp.broadcast_to(cols[j][0][j : j + 1, :], (8, TILE))
            guess = pl.reciprocal(pivot, approx=True)
            fix = 2.0 - pivot * guess
            inverse = guess * fix
            row = jnp.broadcast_to(tiles[0][j : j + 1, :], (8, TILE))
            root = lax.rsqrt(pivot)
            root = root * (1.5 - 0.5 * (pivot * root) * root)
            scale = jnp.where(sub == j, root, scale)
            lead = jnp.where(sub > j, cols[j][0] * guess, 0.0) * fix
            factors = [lead] + [c * inverse for c in cols[j][1:]]
            for l in range(j + 1, 8):
                top = jnp.broadcast_to(cols[l][0][j : j + 1, :], (8, TILE))
                cols[l] = [c - m * top for c, m in zip(cols[l], factors)]
            tiles = [t - m * row for t, m in zip(tiles, factors)]
        dst[8 * g : 8 * g + 8, :] = jnp.where(lane <= sub + 8 * g, tiles[0] * scale, 0.0)
        for q in range(1, len(tiles)):
            src[8 * (g + q) : 8 * (g + q) + 8, :] = tiles[q]


def solve_body(
    mine_ref, other_ref, query_ref, query2_ref, outer_ref, out_ref, a_ref, t_ref, l_ref, b_ref
):
    half = query_ref.shape[0]
    queries = 2 * half
    core = lax.axis_index("core")
    a_ref[pl.ds(core * HALF, HALF)] = mine_ref[...]
    a_ref[pl.ds((1 - core) * HALF, HALF)] = other_ref[...]
    b_ref[:, :half] = query_ref[...].T
    b_ref[:, half:queries] = query2_ref[...].T
    b_ref[:, queries:] = outer_ref[...]
    row = lax.broadcasted_iota(jnp.int32, (TILE, TILE), 0)
    lane = lax.broadcasted_iota(jnp.int32, (TILE, TILE), 1)
    eye = row == lane
    first = a_ref[0]
    holds_count = (row == 1) & (lane == 0)
    token_total = jnp.sum(jnp.where(holds_count, first, 0.0))
    twin = jnp.sum(jnp.where((row == 0) & (lane == 1), first, 0.0))
    a_ref[0] = jnp.where(holds_count, twin, first)
    trace = jnp.zeros((8, TILE), jnp.float32)
    for i in range(SIDE):
        diagonal = jnp.where(eye, a_ref[tile_index(i, i)], 0.0)
        trace = trace + jnp.sum(diagonal.reshape(TILE // 8, 8, TILE), axis=0)
    damping = 0.1 * jnp.sum(trace) / K
    for i in range(SIDE):
        a_ref[tile_index(i, i)] = a_ref[tile_index(i, i)] + jnp.where(eye, damping, 0.0)
    out_ref[...] = jnp.zeros_like(out_ref)

    def eliminate(k):
        right_of = [a_ref[tile_index(k, j)] for j in range(k + 1, SIDE)]
        strip = jnp.concatenate(right_of + [b_ref[TILE * k : TILE * (k + 1), :]], axis=1)
        strip = multiply(left_parts(thirds(l_ref[...]), 1), right_parts(thirds(strip), 0))
        wide = right_parts(thirds(strip), 0)
        width = TILE * (SIDE - 1 - k)

        def flipped(start, stop):
            return left_parts(thirds(strip[:, start:stop].T), 1)

        for j in range(k + 1, SIDE):
            start = TILE * (j - k - 1)
            delta = multiply(flipped(start, start + TILE), wide[:, start:])
            for c in range(j, SIDE):
                a_ref[tile_index(j, c)] -= delta[:, TILE * (c - j) : TILE * (c - j + 1)]
            b_ref[TILE * j : TILE * (j + 1), :] -= delta[:, TILE * (SIDE - j) :]
        out_ref[...] += multiply(flipped(width + queries, strip.shape[1]), wide[:, width : width + queries])

    def step(k, carry):
        t_ref[...] = a_ref[k * SIDE - (k * (k - 1)) // 2]
        invert_factor(t_ref, l_ref)
        for each in range(SIDE):
            pl.when(k == each)(functools.partial(eliminate, each))
        return carry

    lax.fori_loop(0, SIDE, step, 0)
    scores = out_ref[...] * token_total
    is_first = lax.axis_index("z_lo") == 0
    out_ref[:, :half] = jnp.where(is_first, scores[:, :half], scores[:, half:])
    out_ref[:, half:] = jnp.where(is_first, scores[:, half:], scores[:, :half])


def damped_scores(mine, other, my_queries, other_queries, outer_t):
    queries, seqs = 2 * my_queries.shape[0], outer_t.shape[1]
    vmem = pl.BlockSpec(memory_space=pltpu.VMEM)
    return pl.pallas_call(
        solve_body,
        in_specs=[vmem] * 5,
        out_shape=jax.ShapeDtypeStruct((seqs, queries), jnp.float32),
        scratch_shapes=[
            pltpu.VMEM((PACKED, TILE, TILE), jnp.float32),
            pltpu.VMEM((TILE, TILE), jnp.float32),
            pltpu.VMEM((TILE, TILE), jnp.float32),
            pltpu.VMEM((K, queries + seqs), jnp.float32),
        ],
        name="damped_scores",
    )(mine, other, my_queries, other_queries, outer_t)


def members(axes):
    count = 1
    for axis in axes:
        count *= SIZES[axis]
    return count


def scatter_sum(rows, axes):
    peers = members(axes)
    pieces = rows.reshape(peers, -1, TILE)
    return jnp.sum(lax.all_to_all(pieces, axes, 0, 0, tiled=True), axis=0)


def gather_rows(rows, axes):
    peers = members(axes)
    copies = jnp.broadcast_to(rows[None], (peers, *rows.shape))
    return lax.all_to_all(copies, axes, 0, 0, tiled=True).reshape(-1, TILE)


def summed(kept, sent):
    rows = (kept + lax.ppermute(sent, "core", SWAP)).reshape(-1, TILE)
    rows = scatter_sum(rows, NEAR)
    everyone = gather_rows(rows, ("z_hi",)).reshape(SIZES["z_hi"], -1, TILE)
    rows = gather_rows(jnp.sum(everyone, axis=0), NEAR)
    mine = rows.reshape(kept.shape)
    return mine, lax.ppermute(mine, "core", SWAP)


def on_device(hidden_acts, out_grads, loss_mask, proj_in, proj_out, queries):
    other_queries = lax.ppermute(queries, "z_lo", SWAP)
    outer_t, kept, sent = local_gram(hidden_acts, out_grads, loss_mask.T, proj_in, proj_out)
    other_queries, kept, sent = lax.optimization_barrier((other_queries, kept, sent))
    mine, other = summed(kept, sent)
    return damped_scores(mine, other, queries, other_queries, outer_t)


def solution(mesh):
    finer = Mesh(mesh.devices.reshape(4, 4, 4, 2, mesh.shape["query"]), AXES)
    in_specs = (
        P(AXES, None, None),
        P(AXES, None, None),
        P(AXES, None),
        P(),
        P(),
        P("z_lo", None),
    )
    return jax.shard_map(
        on_device, mesh=finer, in_specs=in_specs, out_specs=P(AXES, None), check_vma=False
    )
```

```python
import functools

import jax
import jax.numpy as jnp
from jax import lax
from jax.experimental import pallas as pl
from jax.experimental.pallas import tpu as pltpu
from jax.sharding import Mesh
from jax.sharding import PartitionSpec as P

K = 1024
TILE = 128
SIDE = K // TILE
PACKED = SIDE * (SIDE + 1) // 2
HALF = PACKED // 2
STEPS = 4
AXES = ("z_hi", "x", "y", "core", "z_lo")
SIZES = {"z_hi": 4, "x": 4, "y": 4, "core": 2, "z_lo": 2}
NEAR = ("x", "y", "z_lo")
SWAP = [(0, 1), (1, 0)]


def tile_index(i, j):
    return i * SIDE - i * (i - 1) // 2 + (j - i)


def thirds(x):
    hi = x.astype(jnp.bfloat16)
    rest = x - hi.astype(jnp.float32)
    mid = rest.astype(jnp.bfloat16)
    low = (rest - mid.astype(jnp.float32)).astype(jnp.bfloat16)
    return hi, mid, low


def left_parts(parts, axis):
    hi, mid, low = parts
    return jnp.concatenate([low, mid, hi, mid, hi, hi], axis=axis)


def right_parts(parts, axis):
    hi, mid, low = parts
    return jnp.concatenate([hi, mid, low, hi, mid, hi], axis=axis)


def multiply(a, b):
    return jnp.dot(a, b, preferred_element_type=jnp.float32)


def multiply_rows(a, b):
    return lax.dot_general(a, b, (((1,), (1,)), ((), ())), preferred_element_type=jnp.float32)


def project(x_ref, w_ref, seqs, tokens):
    width = w_ref.shape[0]
    fold = TILE * 2 // width
    blocks = w_ref.shape[1] // TILE
    rows = fold * tokens
    per_seq = blocks * tokens
    left = [
        jnp.concatenate([x_ref[per_seq * s + rows * h : per_seq * s + rows * (h + 1), :] for s in range(seqs)], axis=0)
        for h in range(blocks // fold)
    ]
    right = [
        jnp.concatenate([w_ref[:, TILE * (fold * h + c) : TILE * (fold * h + c + 1)] for c in range(fold)], axis=0)
        for h in range(blocks // fold)
    ]
    all_pairs = multiply_rows(jnp.concatenate(left, axis=1), jnp.concatenate(right, axis=1))
    row = lax.broadcasted_iota(jnp.int32, all_pairs.shape, 0)
    lane = lax.broadcasted_iota(jnp.int32, all_pairs.shape, 1)
    matched = jnp.where((row // tokens) % fold == lane // width, all_pairs, 0.0)
    return jnp.sum(matched.reshape(seqs, rows // 8, 8, fold * width), axis=1).reshape(seqs * 8, fold * width)


def by_token(part_ref, width, token, tokens):
    seqs = part_ref.shape[1] // 8

    def picked(at):
        return jnp.concatenate([part_ref[h, pl.ds(at, seqs, stride=8), :] for h in range(2)], axis=1)

    rows = picked(token)
    for other in range(token + tokens, 8, tokens):
        rows = rows + picked(other)
    row = lax.broadcasted_iota(jnp.int32, (width, rows.shape[1]), 0)
    lane = lax.broadcasted_iota(jnp.int32, (width, rows.shape[1]), 1)
    fold = jnp.where(lane % width == row, 1.0, 0.0).astype(jnp.bfloat16)
    hi, mid, low = thirds(rows)
    return multiply_rows(jnp.concatenate([fold] * 3, axis=1), jnp.concatenate([low, mid, hi], axis=1))


def gram_body(
    act_ref, grad_ref, mask_ref, in_ref, out_ref, outer_ref, kept_ref, sent_ref, a_part, g_part, tiles
):
    tokens = mask_ref.shape[0]
    seqs = outer_ref.shape[1]
    some = seqs // STEPS
    step = pl.program_id(0)
    start = pl.multiple_of(step * some * 8, some * 8)
    for part, x_ref, w_ref in ((a_part, act_ref, in_ref), (g_part, grad_ref, out_ref)):
        found = project(x_ref, w_ref, some, tokens)
        for h in range(2):
            part[h, pl.ds(start, some * 8), :] = found[:, TILE * h : TILE * (h + 1)]

    @pl.when(step == STEPS - 1)
    def _():
        live = mask_ref[...].astype(jnp.float32)
        width = in_ref.shape[0]
        acts = [by_token(a_part, width, t, tokens) for t in range(tokens)]
        grads = [
            by_token(g_part, out_ref.shape[0], t, tokens) * live[t : t + 1, :] for t in range(tokens)
        ]
        for g in range(K // width):
            total = grads[0][g : g + 1, :] * acts[0]
            for t in range(1, tokens):
                total = total + grads[t][g : g + 1, :] * acts[t]
            outer_ref[g * width : (g + 1) * width, :] = total
        parts = thirds(outer_ref[...])
        left, right = left_parts(parts, 1), right_parts(parts, 1)
        for i in range(SIDE):
            strip = multiply_rows(left[TILE * i : TILE * (i + 1), :], right[TILE * i :, :])
            for j in range(i, SIDE):
                tiles[tile_index(i, j)] = strip[:, (j - i) * TILE : (j - i + 1) * TILE]
        row = lax.broadcasted_iota(jnp.int32, (8, TILE), 0)
        lane = lax.broadcasted_iota(jnp.int32, (8, TILE), 1)
        count = jnp.sum(live)
        tiles[0, 0:8, :] = jnp.where((row == 1) & (lane == 0), count, tiles[0, 0:8, :])
        core = lax.axis_index("core")
        kept_ref[...] = tiles[pl.ds(core * HALF, HALF)]
        sent_ref[...] = tiles[pl.ds((1 - core) * HALF, HALF)]


def as_blocks(x):
    seqs, tokens, width = x.shape
    blocks = width // TILE
    return x.reshape(seqs, tokens, blocks, TILE).transpose(0, 2, 1, 3).reshape(seqs * blocks * tokens, TILE)


def local_gram(hidden_acts, out_grads, mask_t, proj_in, proj_out):
    seqs = hidden_acts.shape[0]
    acts, grads = as_blocks(hidden_acts), as_blocks(out_grads)

    def whole(shape):
        return pl.BlockSpec(shape, lambda i: (0,) * len(shape))

    half = (HALF, TILE, TILE)
    return pl.pallas_call(
        gram_body,
        grid=(STEPS,),
        in_specs=[
            pl.BlockSpec((acts.shape[0] // STEPS, TILE), lambda i: (i, 0)),
            pl.BlockSpec((grads.shape[0] // STEPS, TILE), lambda i: (i, 0)),
            whole(mask_t.shape),
            whole(proj_in.shape),
            whole(proj_out.shape),
        ],
        out_specs=(whole((K, seqs)), whole(half), whole(half)),
        out_shape=(
            jax.ShapeDtypeStruct((K, seqs), jnp.float32),
            jax.ShapeDtypeStruct(half, jnp.float32),
            jax.ShapeDtypeStruct(half, jnp.float32),
        ),
        scratch_shapes=[
            pltpu.VMEM((2, seqs * 8, TILE), jnp.float32),
            pltpu.VMEM((2, seqs * 8, TILE), jnp.float32),
            pltpu.VMEM((PACKED, TILE, TILE), jnp.float32),
        ],
        name="local_gram",
    )(acts, grads, mask_t, proj_in, proj_out)


def lanes(tile, start):
    return [jnp.broadcast_to(tile[:, start + j : start + j + 1], (8, TILE)) for j in range(8)]


def across(tile, j):
    return jnp.broadcast_to(tile[j : j + 1, :], (8, TILE))


def reduce_rows(tiles, base):
    lane = lax.broadcasted_iota(jnp.int32, (8, TILE), 1)
    sub = lax.broadcasted_iota(jnp.int32, (8, TILE), 0)
    tiles = list(tiles)
    groups = len(tiles)
    done = []
    corner = lanes(tiles[0], base)
    for g in range(groups):
        more = g + 1 < groups
        at = base + 8 * g
        below = {q: lanes(tiles[q], at) for q in range(g + 1, groups)}
        ahead = lanes(tiles[g], at + 8) if more else []
        following = lanes(tiles[g + 1], at + 8) if more else []
        inside = (lane >= at) & (lane < at + 8)
        for q in range(g + 1, groups):
            tiles[q] = jnp.where(inside, 0.0, tiles[q])
        top = jnp.where(lane == sub + at, 1.0, jnp.where(inside, 0.0, tiles[g]))
        scale = jnp.zeros((8, TILE), jnp.float32)
        for j in range(8):
            pivot = across(corner[j], j)
            guess = pl.reciprocal(pivot, approx=True)
            fix = 2.0 - pivot * guess
            inverse = guess * fix
            root = lax.rsqrt(pivot)
            root = root * (1.5 - 0.5 * (pivot * root) * root)
            scale = jnp.where(sub == j, root, scale)
            lead = jnp.where(sub > j, corner[j] * guess, 0.0) * fix
            row = across(top, j)
            top = top - lead * row
            heads = {l: across(corner[l], j) for l in range(j + 1, 8)}
            for l in range(j + 1, 8):
                corner[l] = corner[l] - lead * heads[l]
            coming = [across(c, j) for c in ahead]
            ahead = [c - lead * r for c, r in zip(ahead, coming)]
            for q in range(g + 1, groups):
                factor = below[q][j] * inverse
                for l in range(j + 1, 8):
                    below[q][l] = below[q][l] - factor * heads[l]
                if q == g + 1:
                    following = [c - factor * r for c, r in zip(following, coming)]
                tiles[q] = tiles[q] - factor * row
        done.append(top * scale)
        corner = following
    return jnp.concatenate(done, axis=0)


def invert_factor(src, dst):
    half = TILE // 2
    row = lax.broadcasted_iota(jnp.int32, (half, TILE), 0)
    lane = lax.broadcasted_iota(jnp.int32, (half, TILE), 1)
    upper = reduce_rows([src[8 * q : 8 * q + 8, :] for q in range(half // 8)], 0)
    kept = jnp.where((lane > row) & (lane < half), 0.0, upper)
    dst[:half, :] = jnp.where(lane < half, kept, 0.0)
    product = lax.dot_general(
        left_parts(thirds(upper), 0),
        right_parts(thirds(kept), 0),
        (((0,), (0,)), ((), ())),
        preferred_element_type=jnp.float32,
    )[half:, :]
    lower = jnp.where(lane < half, 0.0, src[half:, :]) - product
    lower = reduce_rows([lower[8 * q : 8 * q + 8, :] for q in range(half // 8)], half)
    dst[half:, :] = jnp.where(lane <= row + half, lower, 0.0)


def solve_body(
    mine_ref, other_ref, query_ref, query2_ref, outer_ref, out_ref, a_ref, t_ref, l_ref, b_ref
):
    half = query_ref.shape[0]
    queries = 2 * half
    core = lax.axis_index("core")
    a_ref[pl.ds(core * HALF, HALF)] = mine_ref[...]
    a_ref[pl.ds((1 - core) * HALF, HALF)] = other_ref[...]
    b_ref[:, :half] = query_ref[...].T
    b_ref[:, half:queries] = query2_ref[...].T
    b_ref[:, queries:] = outer_ref[...]
    row = lax.broadcasted_iota(jnp.int32, (TILE, TILE), 0)
    lane = lax.broadcasted_iota(jnp.int32, (TILE, TILE), 1)
    eye = row == lane
    first = a_ref[0]
    holds_count = (row == 1) & (lane == 0)
    token_total = jnp.sum(jnp.where(holds_count, first, 0.0))
    twin = jnp.sum(jnp.where((row == 0) & (lane == 1), first, 0.0))
    a_ref[0] = jnp.where(holds_count, twin, first)
    trace = jnp.zeros((8, TILE), jnp.float32)
    for i in range(SIDE):
        diagonal = jnp.where(eye, a_ref[tile_index(i, i)], 0.0)
        trace = trace + jnp.sum(diagonal.reshape(TILE // 8, 8, TILE), axis=0)
    damping = 0.1 * jnp.sum(trace) / K
    for i in range(SIDE):
        a_ref[tile_index(i, i)] = a_ref[tile_index(i, i)] + jnp.where(eye, damping, 0.0)
    out_ref[...] = jnp.zeros_like(out_ref)

    def eliminate(k):
        right_of = [a_ref[tile_index(k, j)] for j in range(k + 1, SIDE)]
        strip = jnp.concatenate(right_of + [b_ref[TILE * k : TILE * (k + 1), :]], axis=1)
        strip = multiply(left_parts(thirds(l_ref[...]), 1), right_parts(thirds(strip), 0))
        wide = right_parts(thirds(strip), 0)
        width = TILE * (SIDE - 1 - k)

        def flipped(start, stop):
            return left_parts(thirds(strip[:, start:stop].T), 1)

        for j in range(k + 1, SIDE):
            start = TILE * (j - k - 1)
            delta = multiply(flipped(start, start + TILE), wide[:, start:])
            for c in range(j, SIDE):
                a_ref[tile_index(j, c)] -= delta[:, TILE * (c - j) : TILE * (c - j + 1)]
            b_ref[TILE * j : TILE * (j + 1), :] -= delta[:, TILE * (SIDE - j) :]
        out_ref[...] += multiply(flipped(width + queries, strip.shape[1]), wide[:, width : width + queries])

    def step(k, carry):
        t_ref[...] = a_ref[k * SIDE - (k * (k - 1)) // 2]
        invert_factor(t_ref, l_ref)
        for each in range(SIDE):
            pl.when(k == each)(functools.partial(eliminate, each))
        return carry

    lax.fori_loop(0, SIDE, step, 0)
    scores = out_ref[...] * token_total
    is_first = lax.axis_index("z_lo") == 0
    out_ref[:, :half] = jnp.where(is_first, scores[:, :half], scores[:, half:])
    out_ref[:, half:] = jnp.where(is_first, scores[:, half:], scores[:, :half])


def damped_scores(mine, other, my_queries, other_queries, outer_t):
    queries, seqs = 2 * my_queries.shape[0], outer_t.shape[1]
    vmem = pl.BlockSpec(memory_space=pltpu.VMEM)
    return pl.pallas_call(
        solve_body,
        in_specs=[vmem] * 5,
        out_shape=jax.ShapeDtypeStruct((seqs, queries), jnp.float32),
        scratch_shapes=[
            pltpu.VMEM((PACKED, TILE, TILE), jnp.float32),
            pltpu.VMEM((TILE, TILE), jnp.float32),
            pltpu.VMEM((TILE, TILE), jnp.float32),
            pltpu.VMEM((K, queries + seqs), jnp.float32),
        ],
        name="damped_scores",
    )(mine, other, my_queries, other_queries, outer_t)


def members(axes):
    count = 1
    for axis in axes:
        count *= SIZES[axis]
    return count


def scatter_sum(rows, axes):
    peers = members(axes)
    pieces = rows.reshape(peers, -1, TILE)
    return jnp.sum(lax.all_to_all(pieces, axes, 0, 0, tiled=True), axis=0)


def gather_rows(rows, axes):
    peers = members(axes)
    copies = jnp.broadcast_to(rows[None], (peers, *rows.shape))
    return lax.all_to_all(copies, axes, 0, 0, tiled=True).reshape(-1, TILE)


def summed(kept, sent):
    rows = (kept + lax.ppermute(sent, "core", SWAP)).reshape(-1, TILE)
    rows = scatter_sum(rows, NEAR)
    everyone = gather_rows(rows, ("z_hi",)).reshape(SIZES["z_hi"], -1, TILE)
    rows = gather_rows(jnp.sum(everyone, axis=0), NEAR)
    mine = rows.reshape(kept.shape)
    return mine, lax.ppermute(mine, "core", SWAP)


def on_device(hidden_acts, out_grads, loss_mask, proj_in, proj_out, queries):
    other_queries = lax.ppermute(queries, "z_lo", SWAP)
    outer_t, kept, sent = local_gram(hidden_acts, out_grads, loss_mask.T, proj_in, proj_out)
    other_queries, kept, sent = lax.optimization_barrier((other_queries, kept, sent))
    mine, other = summed(kept, sent)
    return damped_scores(mine, other, queries, other_queries, outer_t)


def solution(mesh):
    finer = Mesh(mesh.devices.reshape(4, 4, 4, 2, mesh.shape["query"]), AXES)
    in_specs = (
        P(AXES, None, None),
        P(AXES, None, None),
        P(AXES, None),
        P(),
        P(),
        P("z_lo", None),
    )
    return jax.shard_map(
        on_device, mesh=finer, in_specs=in_specs, out_specs=P(AXES, None), check_vma=False
    )
```

```python
import functools

import jax
import jax.numpy as jnp
from jax import lax
from jax.experimental import pallas as pl
from jax.experimental.pallas import tpu as pltpu
from jax.sharding import Mesh
from jax.sharding import PartitionSpec as P


K = 1024
TILE = 128
SIDE = K // TILE
PACKED = SIDE * (SIDE + 1) // 2
HALF = PACKED // 2
STEPS = 4
AXES = ("z_hi", "x", "y", "core", "z_lo")
SIZES = {"z_hi": 4, "x": 4, "y": 4, "core": 2, "z_lo": 2}
NEAR = ("x", "y", "z_lo")
SWAP = [(0, 1), (1, 0)]


def tile_index(i, j):
    return i * SIDE - i * (i - 1) // 2 + (j - i)


def thirds(x):
    hi = x.astype(jnp.bfloat16)
    rest = x - hi.astype(jnp.float32)
    mid = rest.astype(jnp.bfloat16)
    low = (rest - mid.astype(jnp.float32)).astype(jnp.bfloat16)
    return hi, mid, low


def left_parts(parts, axis):
    hi, mid, low = parts
    return jnp.concatenate([low, mid, hi, mid, hi, hi], axis=axis)


def right_parts(parts, axis):
    hi, mid, low = parts
    return jnp.concatenate([hi, mid, low, hi, mid, hi], axis=axis)


def multiply(a, b):
    return jnp.dot(a, b, preferred_element_type=jnp.float32)


def multiply_rows(a, b):
    return lax.dot_general(a, b, (((1,), (1,)), ((), ())), preferred_element_type=jnp.float32)


def project(x_ref, w_ref, seqs, tokens):
    width = w_ref.shape[0]
    fold = TILE * 2 // width
    blocks = w_ref.shape[1] // TILE
    rows = fold * tokens
    per_seq = blocks * tokens
    left = [
        jnp.concatenate([x_ref[per_seq * s + rows * h : per_seq * s + rows * (h + 1), :] for s in range(seqs)], axis=0)
        for h in range(blocks // fold)
    ]
    right = [
        jnp.concatenate([w_ref[:, TILE * (fold * h + c) : TILE * (fold * h + c + 1)] for c in range(fold)], axis=0)
        for h in range(blocks // fold)
    ]
    all_pairs = multiply_rows(jnp.concatenate(left, axis=1), jnp.concatenate(right, axis=1))
    row = lax.broadcasted_iota(jnp.int32, all_pairs.shape, 0)
    lane = lax.broadcasted_iota(jnp.int32, all_pairs.shape, 1)
    matched = jnp.where((row // tokens) % fold == lane // width, all_pairs, 0.0)
    return jnp.sum(matched.reshape(seqs, rows // 8, 8, fold * width), axis=1).reshape(seqs * 8, fold * width)


def by_token(part_ref, width, token, tokens):
    seqs = part_ref.shape[1] // 8

    def picked(at):
        return jnp.concatenate([part_ref[h, pl.ds(at, seqs, stride=8), :] for h in range(2)], axis=1)

    rows = picked(token)
    for other in range(token + tokens, 8, tokens):
        rows = rows + picked(other)
    row = lax.broadcasted_iota(jnp.int32, (width, rows.shape[1]), 0)
    lane = lax.broadcasted_iota(jnp.int32, (width, rows.shape[1]), 1)
    fold = jnp.where(lane % width == row, 1.0, 0.0).astype(jnp.bfloat16)
    hi, mid, low = thirds(rows)
    return multiply_rows(jnp.concatenate([fold] * 3, axis=1), jnp.concatenate([low, mid, hi], axis=1))


def gram_body(
    act_ref, grad_ref, mask_ref, in_ref, out_ref, outer_ref, kept_ref, sent_ref, a_part, g_part, tiles
):
    tokens = mask_ref.shape[0]
    seqs = outer_ref.shape[1]
    some = seqs // STEPS
    step = pl.program_id(0)
    start = pl.multiple_of(step * some * 8, some * 8)
    for part, x_ref, w_ref in ((a_part, act_ref, in_ref), (g_part, grad_ref, out_ref)):
        found = project(x_ref, w_ref, some, tokens)
        for h in range(2):
            part[h, pl.ds(start, some * 8), :] = found[:, TILE * h : TILE * (h + 1)]

    @pl.when(step == STEPS - 1)
    def _():
        live = mask_ref[...].astype(jnp.float32)
        width = in_ref.shape[0]
        acts = [by_token(a_part, width, t, tokens) for t in range(tokens)]
        grads = [
            by_token(g_part, out_ref.shape[0], t, tokens) * live[t : t + 1, :] for t in range(tokens)
        ]
        for g in range(K // width):
            total = grads[0][g : g + 1, :] * acts[0]
            for t in range(1, tokens):
                total = total + grads[t][g : g + 1, :] * acts[t]
            outer_ref[g * width : (g + 1) * width, :] = total
        parts = thirds(outer_ref[...])
        left, right = left_parts(parts, 1), right_parts(parts, 1)
        for i in range(SIDE):
            strip = multiply_rows(left[TILE * i : TILE * (i + 1), :], right[TILE * i :, :])
            for j in range(i, SIDE):
                tiles[tile_index(i, j)] = strip[:, (j - i) * TILE : (j - i + 1) * TILE]
        row = lax.broadcasted_iota(jnp.int32, (8, TILE), 0)
        lane = lax.broadcasted_iota(jnp.int32, (8, TILE), 1)
        count = jnp.sum(live)
        tiles[0, 0:8, :] = jnp.where((row == 1) & (lane == 0), count, tiles[0, 0:8, :])
        core = lax.axis_index("core")
        kept_ref[...] = tiles[pl.ds(core * HALF, HALF)]
        sent_ref[...] = tiles[pl.ds((1 - core) * HALF, HALF)]


def as_blocks(x):
    seqs, tokens, width = x.shape
    blocks = width // TILE
    return x.reshape(seqs, tokens, blocks, TILE).transpose(0, 2, 1, 3).reshape(seqs * blocks * tokens, TILE)


def local_gram(hidden_acts, out_grads, mask_t, proj_in, proj_out):
    seqs = hidden_acts.shape[0]
    acts, grads = as_blocks(hidden_acts), as_blocks(out_grads)

    def whole(shape):
        return pl.BlockSpec(shape, lambda i: (0,) * len(shape))

    half = (HALF, TILE, TILE)
    return pl.pallas_call(
        gram_body,
        grid=(STEPS,),
        in_specs=[
            pl.BlockSpec((acts.shape[0] // STEPS, TILE), lambda i: (i, 0)),
            pl.BlockSpec((grads.shape[0] // STEPS, TILE), lambda i: (i, 0)),
            whole(mask_t.shape),
            whole(proj_in.shape),
            whole(proj_out.shape),
        ],
        out_specs=(whole((K, seqs)), whole(half), whole(half)),
        out_shape=(
            jax.ShapeDtypeStruct((K, seqs), jnp.float32),
            jax.ShapeDtypeStruct(half, jnp.float32),
            jax.ShapeDtypeStruct(half, jnp.float32),
        ),
        scratch_shapes=[
            pltpu.VMEM((2, seqs * 8, TILE), jnp.float32),
            pltpu.VMEM((2, seqs * 8, TILE), jnp.float32),
            pltpu.VMEM((PACKED, TILE, TILE), jnp.float32),
        ],
        name="local_gram",
    )(acts, grads, mask_t, proj_in, proj_out)


def lanes(tile, start):
    return [jnp.broadcast_to(tile[:, start + j : start + j + 1], (8, TILE)) for j in range(8)]


def across(tile, j):
    return jnp.broadcast_to(tile[j : j + 1, :], (8, TILE))


def reduce_rows(tiles, base):
    lane = lax.broadcasted_iota(jnp.int32, (8, TILE), 1)
    sub = lax.broadcasted_iota(jnp.int32, (8, TILE), 0)
    tiles = list(tiles)
    groups = len(tiles)
    done = []
    corner = lanes(tiles[0], base)
    for g in range(groups):
        more = g + 1 < groups
        at = base + 8 * g
        below = {q: lanes(tiles[q], at) for q in range(g + 1, groups)}
        ahead = lanes(tiles[g], at + 8) if more else []
        following = lanes(tiles[g + 1], at + 8) if more else []
        inside = (lane >= at) & (lane < at + 8)
        for q in range(g + 1, groups):
            tiles[q] = jnp.where(inside, 0.0, tiles[q])
        top = jnp.where(lane == sub + at, 1.0, jnp.where(inside, 0.0, tiles[g]))
        scale = jnp.zeros((8, TILE), jnp.float32)
        for j in range(8):
            pivot = across(corner[j], j)
            guess = pl.reciprocal(pivot, approx=True)
            fix = 2.0 - pivot * guess
            inverse = guess * fix
            root = lax.rsqrt(pivot)
            root = root * (1.5 - 0.5 * (pivot * root) * root)
            scale = jnp.where(sub == j, root, scale)
            lead = jnp.where(sub > j, corner[j] * guess, 0.0) * fix
            row = across(top, j)
            top = top - lead * row
            heads = {l: across(corner[l], j) for l in range(j + 1, 8)}
            for l in range(j + 1, 8):
                corner[l] = corner[l] - lead * heads[l]
            coming = [across(c, j) for c in ahead]
            ahead = [c - lead * r for c, r in zip(ahead, coming)]
            for q in range(g + 1, groups):
                factor = below[q][j] * inverse
                for l in range(j + 1, 8):
                    below[q][l] = below[q][l] - factor * heads[l]
                if q == g + 1:
                    following = [c - factor * r for c, r in zip(following, coming)]
                tiles[q] = tiles[q] - factor * row
        done.append(top * scale)
        corner = following
    return jnp.concatenate(done, axis=0)


def invert_factor(src, dst):
    half = TILE // 2
    row = lax.broadcasted_iota(jnp.int32, (half, TILE), 0)
    lane = lax.broadcasted_iota(jnp.int32, (half, TILE), 1)
    upper = reduce_rows([src[8 * q : 8 * q + 8, :] for q in range(half // 8)], 0)
    kept = jnp.where((lane > row) & (lane < half), 0.0, upper)
    dst[:half, :] = jnp.where(lane < half, kept, 0.0)
    product = lax.dot_general(
        left_parts(thirds(upper), 0),
        right_parts(thirds(kept), 0),
        (((0,), (0,)), ((), ())),
        preferred_element_type=jnp.float32,
    )[half:, :]
    lower = jnp.where(lane < half, 0.0, src[half:, :]) - product
    lower = reduce_rows([lower[8 * q : 8 * q + 8, :] for q in range(half // 8)], half)
    dst[half:, :] = jnp.where(lane <= row + half, lower, 0.0)


def solve_body(
    mine_ref, other_ref, query_ref, query2_ref, outer_ref, out_ref, a_ref, t_ref, l_ref, b_ref
):
    half = query_ref.shape[0]
    queries = 2 * half
    core = lax.axis_index("core")
    a_ref[pl.ds(core * HALF, HALF)] = mine_ref[...]
    a_ref[pl.ds((1 - core) * HALF, HALF)] = other_ref[...]
    b_ref[:, :half] = query_ref[...].T
    b_ref[:, half:queries] = query2_ref[...].T
    b_ref[:, queries:] = outer_ref[...]
    row = lax.broadcasted_iota(jnp.int32, (TILE, TILE), 0)
    lane = lax.broadcasted_iota(jnp.int32, (TILE, TILE), 1)
    eye = row == lane
    first = a_ref[0]
    holds_count = (row == 1) & (lane == 0)
    token_total = jnp.sum(jnp.where(holds_count, first, 0.0))
    twin = jnp.sum(jnp.where((row == 0) & (lane == 1), first, 0.0))
    a_ref[0] = jnp.where(holds_count, twin, first)
    trace = jnp.zeros((8, TILE), jnp.float32)
    for i in range(SIDE):
        diagonal = jnp.where(eye, a_ref[tile_index(i, i)], 0.0)
        trace = trace + jnp.sum(diagonal.reshape(TILE // 8, 8, TILE), axis=0)
    damping = 0.1 * jnp.sum(trace) / K
    for i in range(SIDE):
        a_ref[tile_index(i, i)] = a_ref[tile_index(i, i)] + jnp.where(eye, damping, 0.0)
    out_ref[...] = jnp.zeros_like(out_ref)

    def eliminate(k):
        right_of = [a_ref[tile_index(k, j)] for j in range(k + 1, SIDE)]
        strip = jnp.concatenate(right_of + [b_ref[TILE * k : TILE * (k + 1), :]], axis=1)
        strip = multiply(left_parts(thirds(l_ref[...]), 1), right_parts(thirds(strip), 0))
        wide = right_parts(thirds(strip), 0)
        width = TILE * (SIDE - 1 - k)

        def flipped(start, stop):
            return left_parts(thirds(strip[:, start:stop].T), 1)

        for j in range(k + 1, SIDE):
            start = TILE * (j - k - 1)
            delta = multiply(flipped(start, start + TILE), wide[:, start:])
            for c in range(j, SIDE):
                a_ref[tile_index(j, c)] -= delta[:, TILE * (c - j) : TILE * (c - j + 1)]
            b_ref[TILE * j : TILE * (j + 1), :] -= delta[:, TILE * (SIDE - j) :]
        out_ref[...] += multiply(flipped(width + queries, strip.shape[1]), wide[:, width : width + queries])

    def step(k, carry):
        t_ref[...] = a_ref[k * SIDE - (k * (k - 1)) // 2]
        invert_factor(t_ref, l_ref)
        for each in range(SIDE):
            pl.when(k == each)(functools.partial(eliminate, each))
        return carry

    lax.fori_loop(0, SIDE, step, 0)
    scores = out_ref[...] * token_total
    is_first = lax.axis_index("z_lo") == 0
    out_ref[:, :half] = jnp.where(is_first, scores[:, :half], scores[:, half:])
    out_ref[:, half:] = jnp.where(is_first, scores[:, half:], scores[:, :half])


def damped_scores(mine, other, my_queries, other_queries, outer_t):
    queries, seqs = 2 * my_queries.shape[0], outer_t.shape[1]
    vmem = pl.BlockSpec(memory_space=pltpu.VMEM)
    return pl.pallas_call(
        solve_body,
        in_specs=[vmem] * 5,
        out_shape=jax.ShapeDtypeStruct((seqs, queries), jnp.float32),
        scratch_shapes=[
            pltpu.VMEM((PACKED, TILE, TILE), jnp.float32),
            pltpu.VMEM((TILE, TILE), jnp.float32),
            pltpu.VMEM((TILE, TILE), jnp.float32),
            pltpu.VMEM((K, queries + seqs), jnp.float32),
        ],
        name="damped_scores",
    )(mine, other, my_queries, other_queries, outer_t)


def members(axes):
    count = 1
    for axis in axes:
        count *= SIZES[axis]
    return count


def scatter_sum(rows, axes):
    peers = members(axes)
    pieces = rows.reshape(peers, -1, TILE)
    return jnp.sum(lax.all_to_all(pieces, axes, 0, 0, tiled=True), axis=0)


def gather_rows(rows, axes):
    peers = members(axes)
    copies = jnp.broadcast_to(rows[None], (peers, *rows.shape))
    return lax.all_to_all(copies, axes, 0, 0, tiled=True).reshape(-1, TILE)


def exchange_sum(rows):
    peers = SIZES["z_hi"]
    one, two, three = (
        lax.ppermute(rows, "z_hi", [(a, a ^ d) for a in range(peers)]) for d in range(1, peers)
    )
    return (rows + one) + (two + three)


def summed(rows, shape):
    rows = exchange_sum(scatter_sum(rows.reshape(-1, TILE), NEAR))
    mine = gather_rows(rows, NEAR).reshape(shape)
    return mine, lax.ppermute(mine, "core", SWAP)


def on_device(hidden_acts, out_grads, loss_mask, proj_in, proj_out, queries):
    other_queries = lax.ppermute(queries, "z_lo", SWAP)
    outer_t, kept, sent = local_gram(hidden_acts, out_grads, loss_mask.T, proj_in, proj_out)
    both = kept + lax.ppermute(sent, "core", SWAP)
    other_queries, both = lax.optimization_barrier((other_queries, both))
    mine, other = summed(both, kept.shape)
    return damped_scores(mine, other, queries, other_queries, outer_t)


def solution(mesh):
    finer = Mesh(mesh.devices.reshape(4, 4, 4, 2, mesh.shape["query"]), AXES)
    in_specs = (
        P(AXES, None, None),
        P(AXES, None, None),
        P(AXES, None),
        P(),
        P(),
        P("z_lo", None),
    )
    return jax.shard_map(
        on_device, mesh=finer, in_specs=in_specs, out_specs=P(AXES, None), check_vma=False
    )
```
